32 devices in a mesh: gx: 4 (over y, core), gy: 8 (over z, x).
Axes of the slice: x: 2, y: 2, z: 4, core: 2. Of those that a mesh axis runs over, the one named last changes fastest.
Arguments:
- transfer: bfloat16 [512, 75, 128], P(('gx', 'gy')), may hold values from -6 to 6
- positions: float32 [512, 3, 128], P(('gx', 'gy')), may hold values from -4 to 4
- normals: float32 [512, 3, 128], P(('gx', 'gy')), may hold values from -4 to 4
- area: float32 [512, 128], P(('gx', 'gy')), may hold values from 0.06 to 3
- albedo: float32 [512, 3, 128], P(('gx', 'gy')), may hold values from 0.3 to 0.9
- pairs: int32 [512, 40], P(('gx', 'gy')), may hold values from 0 to 511, as said below
- home: int32 [512], replicated, may hold values from 0 to 511, as said below
Outputs:
- bounce_one: bfloat16 [512, 75, 128], P(('gx', 'gy'))
- bounce_two: bfloat16 [512, 75, 128], P(('gx', 'gy'))
- energies: float32 [2], replicated
The draws below stay inside these ranges and needn't reach their ends.
Inputs may be any that keep to these rules, and one draw needn't show every extreme that they name: `home`: A permutation; the block in slot s is held by device s // 16, devices counted gx major. `pairs`: the first 16 entries of a row name blocks held by the same device as the row's slot, the other 24 name blocks held by other devices. Over the rows of one device, the far entries name at most 2 distinct blocks of any one other device, and exactly 2 of some. Ids may repeat within a row; each entry counts.
All inputs are finite; a program needn't handle non-finite values.
Results may differ from the reference program's by a relative error of at most 0.02.
Values may be sent and summed in bfloat16 or wider, within the bound.
A program may use at most 128 MiB of HBM per device.

```python
import jax
import jax.numpy as jnp
from jax import lax

BLK_DEV = 16
VERT = 128
COLORS = 3
NEAR = 16
FAR = 24
CAP = 2
CH = 75
BLOCKS = 512


def layout_tables(key):
    devices_all = BLOCKS // BLK_DEV
    home = jax.random.permutation(jax.random.fold_in(key, 11), BLOCKS).astype(jnp.int32)
    inverse = jnp.argsort(home, stable=True).astype(jnp.int32)
    keys = jax.random.split(jax.random.fold_in(key, 12), 4)
    slot_all = jnp.arange(BLOCKS, dtype=jnp.int32)
    device_of = slot_all // BLK_DEV
    near_local = jax.random.randint(keys[0], (BLOCKS, NEAR), 0, BLK_DEV, dtype=jnp.int32)
    near_slot = device_of[:, None] * BLK_DEV + near_local
    offset = jax.random.randint(keys[1], (BLOCKS, FAR), 1, devices_all, dtype=jnp.int32)
    column = jnp.arange(FAR, dtype=jnp.int32)[None, :]
    forced = (slot_all % BLK_DEV == 0)[:, None] & (column < CAP)
    offset = jnp.where(forced, 1, offset)
    pick_k = jax.random.randint(keys[2], (BLOCKS, FAR), 0, CAP, dtype=jnp.int32)
    pick_k = jnp.where(forced, column, pick_k)
    owner_dev = (device_of[:, None] + offset) % devices_all
    start_tab = jax.random.randint(keys[3], (devices_all, devices_all), 0, BLK_DEV, dtype=jnp.int32)
    local_idx = (start_tab[device_of[:, None], owner_dev] + pick_k) % BLK_DEV
    far_slot = owner_dev * BLK_DEV + local_idx
    source_slot = jnp.concatenate([near_slot, far_slot], axis=1)
    pairs = jnp.take(inverse, source_slot, axis=0).astype(jnp.int32)
    return (home, pairs)


def draw_home(key, part):
    return layout_tables(key)[0]


def draw_pairs(key, part):
    return layout_tables(key)[1]


def draw_area(key, part):
    ramp = jnp.arange(BLOCKS, dtype=jnp.float32)[:, None] / (BLOCKS - 1)
    logs = jax.random.uniform(key, (BLOCKS, VERT), jnp.float32, jnp.log(0.2), jnp.log(2.0))
    return jnp.exp(logs) * (0.5 + ramp)


def shard_levels(own_key, extent, cuts, least, largest):
    gain, own = 1.0, jax.random.fold_in(own_key, 6)
    for position, blocks in cuts:
        draws = jnp.exp(jax.random.uniform(jax.random.fold_in(own, position), (blocks,), jnp.float32, least / len(cuts), largest / len(cuts)))
        gain = gain * jnp.repeat(draws, extent[position] // blocks).reshape([-1 if axis == position else 1 for axis in range(len(extent))])
    return gain


def bell_draw(stream_key, extent, spread, bound, cuts=(), kind=jnp.bfloat16):
    values = spread * jax.random.normal(stream_key, extent, jnp.float32)
    if cuts:
        values = values * shard_levels(stream_key, extent, cuts, -0.22, 0.18)
    return jnp.clip(values, -bound, bound).astype(kind)


def setup_inputs(seed: int = 0) -> dict:
    key_list = jax.random.split(jax.random.key(seed), 8)
    return {
        "transfer": bell_draw(key_list[0], (BLOCKS, CH, VERT), 1.0, 6.0, ((0, 32),)),
        "positions": bell_draw(key_list[1], (BLOCKS, 3, VERT), 1.0, 4.0, ((0, 32),), jnp.float32),
        "normals": bell_draw(key_list[2], (BLOCKS, 3, VERT), 1.0, 4.0, ((0, 32),), jnp.float32),
        "area": draw_area(jax.random.fold_in(key_list[7], 71), 0),
        "albedo": jnp.clip(0.3 + 0.59999996 * jax.random.uniform(key_list[4], (BLOCKS, COLORS, VERT), jnp.float32) ** shard_levels(key_list[4], (BLOCKS, COLORS, VERT), ((0, 32),), -0.2, 0.2), 0.3, 0.9),
        "pairs": draw_pairs(jax.random.fold_in(key_list[7], 71), 0),
        "home": draw_home(jax.random.fold_in(key_list[7], 71), 0),
    }


batch_blocks = 4


def form_tiles(recv_pos, recv_nrm, src_pos, src_nrm, src_area):
    distance = None
    along_p = None
    along_q = None
    for axis_id in range(3):
        gap_vec = src_pos[:, :, axis_id, None, :] - recv_pos[:, None, axis_id, :, None]
        near_term = recv_nrm[:, None, axis_id, :, None] * gap_vec
        far_term = src_nrm[:, :, axis_id, None, :] * gap_vec
        if distance is None:
            distance = gap_vec * gap_vec
            along_p = near_term
            along_q = far_term
        else:
            distance = distance + gap_vec * gap_vec
            along_p = along_p + near_term
            along_q = along_q + far_term
    soft_sq = distance + 1.0
    transfer_factors = jnp.maximum(along_p, 0.0) * jnp.maximum(-along_q, 0.0) * src_area[:, :, None, :] / (jnp.pi * soft_sq * soft_sq)
    return transfer_factors.astype(jnp.bfloat16)


def reflect_all(source_rows, src_positions, src_normals, src_area, pair_row_list, recv_positions, recv_normals):
    turns = pair_row_list.shape[0] // batch_blocks

    def group_term(group_id):
        first_row = group_id * batch_blocks
        picked_rows = lax.dynamic_slice_in_dim(pair_row_list, first_row, batch_blocks, 0)
        recv_pos = lax.dynamic_slice_in_dim(recv_positions, first_row, batch_blocks, 0)
        recv_nrm = lax.dynamic_slice_in_dim(recv_normals, first_row, batch_blocks, 0)
        transfer_factors = form_tiles(recv_pos, recv_nrm, jnp.take(src_positions, picked_rows, axis=0),
                             jnp.take(src_normals, picked_rows, axis=0), jnp.take(src_area, picked_rows, axis=0))
        collected_values = jnp.take(source_rows, picked_rows, axis=0)
        return jnp.einsum('wxmy,wxsy->wms', collected_values.astype(jnp.float32), transfer_factors.astype(jnp.float32))

    summed = lax.map(group_term, jnp.arange(turns, dtype=jnp.int32))
    return summed.reshape((pair_row_list.shape[0],) + source_rows.shape[1:])


def apply_albedo(summed, albedo):
    blocks_here, channels, verts = summed.shape
    shaped = summed.reshape(blocks_here, COLORS, channels // COLORS, verts) * albedo[:, :, None, :]
    return shaped.reshape(blocks_here, channels, verts)


def reference(transfer, positions, normals, area, albedo, pairs, home):
    slot_ids = jnp.take(home, pairs, axis=0)
    first_bounce = apply_albedo(reflect_all(transfer, positions, normals, area, slot_ids, positions, normals), albedo)
    bounce_one = first_bounce.astype(jnp.bfloat16)
    second_bounce = apply_albedo(reflect_all(bounce_one, positions, normals, area, slot_ids, positions, normals), albedo)
    bounce_two = second_bounce.astype(jnp.bfloat16)
    inv_count = 1.0 / (BLOCKS * VERT * CH)
    energy_one = jnp.sum(area[:, None, :] * first_bounce * first_bounce) * inv_count
    energy_two = jnp.sum(area[:, None, :] * second_bounce * second_bounce) * inv_count
    energies = jnp.stack([energy_one, energy_two]).astype(jnp.float32)
    return bounce_one, bounce_two, energies
```

```python
import functools

import jax
import jax.numpy as jnp
from jax import lax
from jax.experimental import pallas as pl
from jax.experimental.pallas import tpu as pltpu
from jax.sharding import PartitionSpec as P

COLORS = 3
NEAR = 16
CAP = 2
AXES = ("gx", "gy")
VMEM_LIMIT = 48 * 1024 * 1024


def split3(f):
    hi = f.astype(jnp.bfloat16).astype(jnp.float32)
    rest = f - hi
    mid = rest.astype(jnp.bfloat16).astype(jnp.float32)
    return hi, mid, rest - mid


def source_features(pos, nrm, area):
    lanes = pos.shape[1]
    m = nrm * (area * (1.0 / jnp.pi))
    sq = jnp.sum(pos * pos, axis=0, keepdims=True)
    d = -jnp.sum(m * pos, axis=0, keepdims=True)
    feat = jnp.concatenate([pos, sq, m, d], axis=0)
    hi, mid, lo = split3(feat)
    ones = jnp.ones((8, lanes), jnp.float32)
    half = jnp.concatenate([hi, hi, hi, mid, mid, lo, ones, jnp.zeros_like(ones)], axis=0)
    return jnp.concatenate([half, half], axis=0).T


def receiver_weights(pos, nrm):
    lanes = pos.shape[1]
    zero3 = jnp.zeros((3, lanes), jnp.float32)
    zero1 = jnp.zeros((1, lanes), jnp.float32)
    one1 = jnp.ones((1, lanes), jnp.float32)
    zero5 = jnp.zeros((5, lanes), jnp.float32)
    zero8 = jnp.zeros((8, lanes), jnp.float32)

    def column(feat, const):
        hi, mid, lo = split3(feat)
        chi, cmid, clo = split3(const)
        return jnp.concatenate(
            [hi, mid, lo, hi, mid, hi, jnp.concatenate([chi, cmid, clo, zero5], axis=0), zero8],
            axis=0,
        )

    dist = column(
        jnp.concatenate([-2.0 * pos, one1, zero3, zero1], axis=0),
        jnp.sum(pos * pos, axis=0, keepdims=True) + 1.0,
    )
    along_p = column(
        jnp.concatenate([nrm, zero1, zero3, zero1], axis=0),
        -jnp.sum(nrm * pos, axis=0, keepdims=True),
    )
    along_q = column(jnp.concatenate([zero3, zero1, pos, one1], axis=0), zero1)
    return jnp.concatenate([dist, along_p, along_q], axis=1)


def fill_tables(geom, count, even, odd):
    def one(t, carry):
        rows = source_features(*geom(t))
        lane = lax.broadcasted_iota(jnp.int32, rows.shape, 1)
        even[t] = jnp.where(lane < 64, rows, 0.0).astype(jnp.bfloat16)
        odd[t] = jnp.where(lane < 64, 0.0, rows).astype(jnp.bfloat16)
        return carry

    lax.fori_loop(0, count, one, 0)


def row_tiles(rows_ref, slot, count, weights, even, odd, table, lhs, tiles):
    v = tiles.shape[-1]

    def four(i, carry):
        t = [rows_ref[slot, i * 4 + j] for j in range(4)]
        x = jnp.concatenate([even[t[0]] + odd[t[1]], even[t[2]] + odd[t[3]]], axis=0)
        g = jnp.dot(x, weights, preferred_element_type=jnp.float32)
        for j in range(4):
            r, c = (j // 2) * v, (j % 2) * 3 * v
            dist = g[r : r + v, c : c + v]
            ap = g[r : r + v, c + v : c + 2 * v]
            aq = g[r : r + v, c + 2 * v : c + 3 * v]
            f = jnp.maximum(ap, 0.0) * jnp.maximum(aq, 0.0) / (dist * dist)
            at = pl.multiple_of((i * 4 + j) * v, v)
            tiles[0, pl.ds(at, v), :] = f.astype(jnp.bfloat16)
            lhs[:, pl.ds(at, v)] = table[t[j], 0 : lhs.shape[0], :]
        return carry

    lax.fori_loop(0, count // 4, four, 0)


def gather_rows(rows_ref, slot, count, table, lhs, v):
    for j in range(count):
        lhs[:, j * v : (j + 1) * v] = table[rows_ref[slot, j], 0 : lhs.shape[0], :]


def block_diag(w):
    z = jnp.zeros_like(w)
    return jnp.concatenate(
        [jnp.concatenate([w, z], axis=1), jnp.concatenate([z, w], axis=1)], axis=0
    ).astype(jnp.bfloat16)


def albedo_rows(alb, rows, per_color):
    r = lax.broadcasted_iota(jnp.int32, (rows, alb.shape[1]), 0)
    out = jnp.broadcast_to(alb[COLORS - 1 : COLORS, :], (rows, alb.shape[1]))
    for c in range(COLORS - 2, -1, -1):
        out = jnp.where(r < (c + 1) * per_color, alb[c : c + 1, :], out)
    return out


def near_kernel(rows_ref, pos, nrm, area, table, tiles, acc, even, odd, lhs):
    s = pl.program_id(0)

    @pl.when(s == 0)
    def _():
        fill_tables(lambda t: (pos[t], nrm[t], area[t]), even.shape[0], even, odd)

    weights = block_diag(receiver_weights(pos[s], nrm[s]))
    row_tiles(rows_ref, s, rows_ref.shape[1], weights, even, odd, table, lhs, tiles)
    acc[0] = jnp.dot(lhs[...], tiles[0], preferred_element_type=jnp.float32)


def finish(total, s, alb, area, ch, out, energy):
    val = total * albedo_rows(alb, total.shape[0], ch // COLORS)
    r = lax.broadcasted_iota(jnp.int32, val.shape, 0)
    part = jnp.sum(jnp.where(r < ch, val * val * area, 0.0), axis=0, keepdims=True)
    energy[...] = jnp.where(s == 0, part, energy[...] + part)
    return val.astype(jnp.bfloat16)


def far_kernel(
    ch, rows_ref, pos, nrm, area, alb, near_acc, table, tiles, out, energy, even, odd, lhs
):
    s = pl.program_id(0)

    def geom(t):
        g = table[t, ch:, :].astype(jnp.float32)
        return g[0:3] + g[3:6], g[6:9] + g[9:12], g[12:13]

    @pl.when(s == 0)
    def _():
        fill_tables(geom, even.shape[0], even, odd)

    weights = block_diag(receiver_weights(pos[s], nrm[s]))
    row_tiles(rows_ref, s, rows_ref.shape[1], weights, even, odd, table, lhs, tiles)
    total = near_acc[0] + jnp.dot(lhs[...], tiles[0], preferred_element_type=jnp.float32)
    out[0] = finish(total, s, alb[s], area[s], ch, out, energy)


def near_second(rows_ref, table, tiles, acc, lhs):
    s = pl.program_id(0)
    gather_rows(rows_ref, s, rows_ref.shape[1], table, lhs, tiles.shape[-1])
    acc[0] = jnp.dot(lhs[...], tiles[0], preferred_element_type=jnp.float32)


def far_second(ch, rows_ref, area, alb, near_acc, table, tiles, out, energy, lhs):
    s = pl.program_id(0)
    gather_rows(rows_ref, s, rows_ref.shape[1], table, lhs, tiles.shape[-1])
    total = near_acc[0] + jnp.dot(lhs[...], tiles[0], preferred_element_type=jnp.float32)
    out[0] = finish(total, s, alb[s], area[s], ch, out, energy)[0:ch]


def whole(x):
    nd = len(x.shape)
    return pl.BlockSpec(x.shape, lambda s: (0,) * nd)


def per_slot(shape):
    nd = len(shape)
    return pl.BlockSpec((1,) + tuple(shape[1:]), lambda s: (s,) + (0,) * (nd - 1))


def call(kernel, name, ins, sliced, outs, scratch, flops):
    specs = [pl.BlockSpec(memory_space=pltpu.SMEM)]
    for i, x in enumerate(ins[1:], 1):
        specs.append(per_slot(x.shape) if i in sliced else whole(x))
    return pl.pallas_call(
        kernel,
        name=name,
        grid=(ins[0].shape[0],),
        in_specs=specs,
        out_specs=[per_slot(o.shape) if len(o.shape) == 3 else whole(o) for o in outs],
        out_shape=outs,
        scratch_shapes=scratch,
        compiler_params=pltpu.CompilerParams(vmem_limit_bytes=VMEM_LIMIT),
        cost_estimate=pl.CostEstimate(flops=flops, bytes_accessed=1 << 20, transcendentals=0),
    )(*ins)


def body(transfer, positions, normals, area, albedo, pairs, home):
    n = lax.axis_size(AXES)
    me = lax.axis_index(AXES)
    b, ch, v = transfer.shape
    far = pairs.shape[1] - NEAR
    rows = -(-ch // 16) * 16
    bf16, f32 = jnp.bfloat16, jnp.float32

    ids = jnp.arange(home.shape[0], dtype=jnp.int32)
    slot_ids = jnp.sum(jnp.where(pairs[:, :, None] == ids, home, 0), axis=2)
    near_rows = slot_ids[:, :NEAR] - me * b
    far_ids = slot_ids[:, NEAR:]
    owner = far_ids // b
    local = far_ids - owner * b
    devs = jnp.arange(n, dtype=jnp.int32)
    mine = owner[:, :, None] == devs
    low = jnp.min(jnp.where(mine, local[:, :, None], b - 1), axis=(0, 1))
    high = jnp.max(jnp.where(mine, local[:, :, None], 0), axis=(0, 1))
    low_of = jnp.sum(jnp.where(mine, low, 0), axis=2)
    far_rows = owner * CAP + (local > low_of).astype(jnp.int32)
    asked = lax.all_to_all(
        jnp.stack([low, high], axis=1), AXES, split_axis=0, concat_axis=0, tiled=True
    ).reshape(-1)

    def hi_mid(x):
        hi = lax.reduce_precision(x, 8, 7)
        return [hi.astype(bf16), (x - hi).astype(bf16)]

    packed = jnp.concatenate(
        [transfer] + hi_mid(positions) + hi_mid(normals) + [area[:, None, :].astype(bf16)], axis=1
    )
    sent = jnp.take(packed, asked, axis=0)
    arrived = lax.all_to_all(sent, AXES, split_axis=0, concat_axis=0, tiled=True)

    area3 = area[:, None, :]
    lhs = lambda j: pltpu.VMEM((rows, j * v), bf16)
    tab = lambda t: pltpu.VMEM((t, v, v), bf16)
    acc_shape = jax.ShapeDtypeStruct((b, rows, v), f32)
    en_shape = jax.ShapeDtypeStruct((1, v), f32)
    near_tiles, near_acc = call(
        near_kernel, "near_first",
        (near_rows, positions, normals, area3, packed), (),
        [jax.ShapeDtypeStruct((b, NEAR * v, v), bf16), acc_shape],
        [tab(b), tab(b), lhs(NEAR)],
        2 * b * NEAR * v * v * 400,
    )
    far_tiles, one, en_one = call(
        functools.partial(far_kernel, ch), "far_first",
        (far_rows, positions, normals, area3, albedo, near_acc, arrived), (5,),
        [
            jax.ShapeDtypeStruct((b, far * v, v), bf16),
            jax.ShapeDtypeStruct((b, rows, v), bf16),
            en_shape,
        ],
        [tab(n * CAP), tab(n * CAP), lhs(far)],
        2 * b * far * v * v * 400,
    )
    sent2 = jnp.take(one, asked, axis=0)
    arrived2 = lax.all_to_all(sent2, AXES, split_axis=0, concat_axis=0, tiled=True)
    (near2,) = call(
        near_second, "near_second", (near_rows, one, near_tiles), (2,),
        [acc_shape], [lhs(NEAR)], 2 * b * NEAR * v * v * rows,
    )
    two, en_two = call(
        functools.partial(far_second, ch), "far_second",
        (far_rows, area3, albedo, near2, arrived2, far_tiles), (3, 5),
        [jax.ShapeDtypeStruct((b, ch, v), bf16), en_shape],
        [lhs(far)], 2 * b * far * v * v * rows,
    )
    part = jnp.stack([jnp.sum(en_one), jnp.sum(en_two)])
    parts = lax.all_to_all(
        jnp.broadcast_to(part, (n, 2)), AXES, split_axis=0, concat_axis=0, tiled=True
    )
    energies = jnp.sum(parts, axis=0) * (1.0 / (n * b * v * ch))
    return one[:, :ch], two, energies


def solution(mesh):
    return jax.shard_map(
        body,
        mesh=mesh,
        in_specs=(
            P(AXES, None, None),
            P(AXES, None, None),
            P(AXES, None, None),
            P(AXES, None),
            P(AXES, None, None),
            P(AXES, None),
            P(),
        ),
        out_specs=(P(AXES, None, None), P(AXES, None, None), P()),
        check_vma=False,
    )
```

```python
import functools

import jax
import jax.numpy as jnp
from jax import lax
from jax.experimental import pallas as pl
from jax.experimental.pallas import tpu as pltpu
from jax.sharding import PartitionSpec as P

COLORS = 3
NEAR = 16
CAP = 2
AXES = ("gx", "gy")
GEO = 16
VMEM_LIMIT = 62 * 1024 * 1024
MESH = pl.DeviceIdType.MESH


def split3(f):
    hi = f.astype(jnp.bfloat16).astype(jnp.float32)
    rest = f - hi
    mid = rest.astype(jnp.bfloat16).astype(jnp.float32)
    return hi, mid, rest - mid


def source_features(pos, nrm, area):
    lanes = pos.shape[1]
    m = nrm * (area * (1.0 / jnp.pi))
    sq = jnp.sum(pos * pos, axis=0, keepdims=True)
    d = -jnp.sum(m * pos, axis=0, keepdims=True)
    feat = jnp.concatenate([pos, sq, m, d], axis=0)
    hi, mid, lo = split3(feat)
    ones = jnp.ones((8, lanes), jnp.float32)
    half = jnp.concatenate([hi, hi, hi, mid, mid, lo, ones, jnp.zeros_like(ones)], axis=0)
    return jnp.concatenate([half, half], axis=0).T


def receiver_weights(pos, nrm):
    lanes = pos.shape[1]
    zero3 = jnp.zeros((3, lanes), jnp.float32)
    zero1 = jnp.zeros((1, lanes), jnp.float32)
    one1 = jnp.ones((1, lanes), jnp.float32)
    zero5 = jnp.zeros((5, lanes), jnp.float32)
    zero8 = jnp.zeros((8, lanes), jnp.float32)

    def column(feat, const):
        hi, mid, lo = split3(feat)
        chi, cmid, clo = split3(const)
        return jnp.concatenate(
            [hi, mid, lo, hi, mid, hi, jnp.concatenate([chi, cmid, clo, zero5], axis=0), zero8],
            axis=0,
        )

    dist = column(
        jnp.concatenate([-2.0 * pos, one1, zero3, zero1], axis=0),
        jnp.sum(pos * pos, axis=0, keepdims=True) + 1.0,
    )
    along_p = column(
        jnp.concatenate([nrm, zero1, zero3, zero1], axis=0),
        -jnp.sum(nrm * pos, axis=0, keepdims=True),
    )
    along_q = column(jnp.concatenate([zero3, zero1, pos, one1], axis=0), zero1)
    return jnp.concatenate([dist, along_p, along_q], axis=1)


def block_diag(w):
    z = jnp.zeros_like(w)
    return jnp.concatenate(
        [jnp.concatenate([w, z], axis=1), jnp.concatenate([z, w], axis=1)], axis=0
    ).astype(jnp.bfloat16)


def albedo_rows(alb, rows, per_color):
    r = lax.broadcasted_iota(jnp.int32, (rows, alb.shape[1]), 0)
    out = jnp.broadcast_to(alb[COLORS - 1 : COLORS, :], (rows, alb.shape[1]))
    for c in range(COLORS - 2, -1, -1):
        out = jnp.where(r < (c + 1) * per_color, alb[c : c + 1, :], out)
    return out


def fill_table(geom, count, feats):
    def one(t, carry):
        feats[t] = source_features(*geom(t)).astype(jnp.bfloat16)
        return carry

    lax.fori_loop(0, count, one, 0)


def row_tiles(rows_ref, slot, base, weights, feats, tiles):
    v = tiles.shape[-1]
    first = lax.broadcasted_iota(jnp.int32, (v, v), 1) < v // 2
    for i in range(rows_ref.shape[1] // 4):
        t = [rows_ref[slot, i * 4 + j] for j in range(4)]
        x = jnp.concatenate(
            [
                jnp.where(first, feats[t[0]], feats[t[1]]),
                jnp.where(first, feats[t[2]], feats[t[3]]),
            ],
            axis=0,
        )
        g = jnp.dot(x, weights, preferred_element_type=jnp.float32)
        for j in range(4):
            r, c = (j // 2) * v, (j % 2) * 3 * v
            dist = g[r : r + v, c : c + v]
            ap = g[r : r + v, c + v : c + 2 * v]
            aq = g[r : r + v, c + 2 * v : c + 3 * v]
            f = jnp.maximum(ap, 0.0) * jnp.maximum(aq, 0.0) / (dist * dist)
            at = base + (i * 4 + j) * v
            tiles[slot, at : at + v, :] = f.astype(jnp.bfloat16)


def contract(rows_ref, slot, base, load, lhs, tiles):
    v = tiles.shape[-1]
    count = rows_ref.shape[1]
    for j in range(count):
        lhs[:, j * v : (j + 1) * v] = load(rows_ref[slot, j])
    return jnp.dot(
        lhs[:, 0 : count * v],
        tiles[slot, base : base + count * v, :],
        preferred_element_type=jnp.float32,
    )


def bounce_kernel(
    n, ny,
    near_rows, far_rows, asked,
    transfer, pos, nrm, area, alb,
    one_ref, two_ref, energy_ref,
    local, geo_local, geo_out, geo_in, box_out, box_in, box_in2,
    near_feats, far_feats, tiles, lhs, acc, one, en, en_in,
    gs, gr, rs, rr, ss, sr, e1s, e1r, e2s, e2r,
):
    bf16, f32 = jnp.bfloat16, jnp.float32
    me = lax.axis_index("gx") * ny + lax.axis_index("gy")
    b, ch, v = transfer.shape
    rows = local.shape[1]
    near = near_rows.shape[1]

    def peer(d):
        t = lax.rem(me + d, n)
        return t, (t // ny, lax.rem(t, ny))

    def each_peer(fn):
        def step(d, carry):
            fn(d)
            return carry

        lax.fori_loop(1, n, step, 0)

    def copies(src, dst, send, recv):
        def make(d):
            t, dev = peer(d)
            return pltpu.make_async_remote_copy(
                src_ref=src(t), dst_ref=dst, send_sem=send.at[d], recv_sem=recv.at[d],
                device_id=dev, device_id_type=MESH,
            )

        return make

    def pair(ref, t):
        return ref.at[pl.ds(t * CAP, CAP)]

    geo_cp = copies(lambda t: pair(geo_out, t), pair(geo_in, me), gs, gr)
    rad_cp = copies(lambda t: pair(box_out, t), pair(box_in, me), rs, rr)
    sec_cp = copies(lambda t: pair(box_out, t), pair(box_in2, me), ss, sr)
    e1_cp = copies(lambda t: en.at[0], en_in.at[0, me], e1s, e1r)
    e2_cp = copies(lambda t: en.at[1], en_in.at[1, me], e2s, e2r)

    barrier = pltpu.get_barrier_semaphore()
    each_peer(lambda d: pl.semaphore_signal(barrier, inc=1, device_id=peer(d)[1], device_id_type=MESH))

    def stage(t, carry):
        local[t] = jnp.concatenate(
            [transfer[t], jnp.zeros((rows - ch, v), bf16)], axis=0
        )
        p_hi, p_mid, _ = split3(pos[t])
        n_hi, n_mid, _ = split3(nrm[t])
        geo_local[t] = jnp.concatenate(
            [p_hi, p_mid, n_hi, n_mid, area[t], jnp.zeros((GEO - 13, v), f32)], axis=0
        ).astype(bf16)
        return carry

    lax.fori_loop(0, b, stage, 0)

    def pack(source, out):
        def step(t, carry):
            for k in range(CAP):
                out[t * CAP + k] = source[asked[t * CAP + k]]
            return carry

        lax.fori_loop(0, n, step, 0)

    pack(geo_local, geo_out)
    pack(local, box_out)
    for box in (geo_in, box_in, box_in2):
        for k in range(CAP):
            box[me * CAP + k] = jnp.zeros(box.shape[1:], bf16)
    pl.semaphore_wait(barrier, n - 1)
    each_peer(lambda d: geo_cp(d).start())
    each_peer(lambda d: rad_cp(d).start())

    def weights_of(s):
        return block_diag(receiver_weights(pos[s], nrm[s]))

    fill_table(lambda t: (pos[t], nrm[t], area[t]), b, near_feats)

    def near_slot(s, carry):
        row_tiles(near_rows, s, 0, weights_of(s), near_feats, tiles)
        acc[s] = contract(near_rows, s, 0, lambda t: local[t], lhs, tiles)
        return carry

    lax.fori_loop(0, b, near_slot, 0)
    each_peer(lambda d: geo_cp(d).wait())

    def far_geom(t):
        g = geo_in[t].astype(f32)
        return g[0:3] + g[3:6], g[6:9] + g[9:12], g[12:13]

    fill_table(far_geom, n * CAP, far_feats)

    def far_slot(s, carry):
        row_tiles(far_rows, s, near * v, weights_of(s), far_feats, tiles)
        return carry

    lax.fori_loop(0, b, far_slot, 0)
    each_peer(lambda d: rad_cp(d).wait())

    def finish(s, box, e):
        total = acc[s] + contract(far_rows, s, near * v, lambda t: box[t], lhs, tiles)
        val = total * albedo_rows(alb[s], rows, ch // COLORS)
        r = lax.broadcasted_iota(jnp.int32, val.shape, 0)
        part = jnp.sum(jnp.where(r < ch, val * val * area[s], 0.0), axis=0, keepdims=True)
        return val.astype(bf16), e + part

    def first_slot(s, e):
        val, e = finish(s, box_in, e)
        one[s] = val
        one_ref[s] = val[0:ch]
        return e

    zero = jnp.zeros((1, v), f32)
    row0 = lax.broadcasted_iota(jnp.int32, (8, v), 0) == 0
    e1 = lax.fori_loop(0, b, first_slot, zero)
    pack(one, box_out)
    each_peer(lambda d: sec_cp(d).start())
    en[0] = jnp.where(row0, e1, 0.0)
    en_in[0, me] = en[0]

    def near_again(s, carry):
        acc[s] = contract(near_rows, s, 0, lambda t: one[t], lhs, tiles)
        return carry

    lax.fori_loop(0, b, near_again, 0)
    each_peer(lambda d: e1_cp(d).start())
    each_peer(lambda d: sec_cp(d).wait())

    def second_slot(s, e):
        val, e = finish(s, box_in2, e)
        two_ref[s] = val[0:ch]
        return e

    e2 = lax.fori_loop(0, b, second_slot, zero)
    en[1] = jnp.where(row0, e2, 0.0)
    en_in[1, me] = en[1]
    each_peer(lambda d: e2_cp(d).start())
    each_peer(lambda d: e1_cp(d).wait())
    each_peer(lambda d: e2_cp(d).wait())
    energy_ref[...] = jnp.sum(en_in[...], axis=1)


def body(transfer, positions, normals, area, albedo, pairs, home):
    n = lax.axis_size(AXES)
    me = lax.axis_index(AXES)
    b, ch, v = transfer.shape
    far = pairs.shape[1] - NEAR
    rows = -(-ch // 16) * 16
    bf16, f32 = jnp.bfloat16, jnp.float32

    ids = jnp.arange(home.shape[0], dtype=jnp.int32)
    slot_ids = jnp.sum(jnp.where(pairs[:, :, None] == ids, home, 0), axis=2)
    near_rows = slot_ids[:, :NEAR] - me * b
    far_ids = slot_ids[:, NEAR:]
    owner = far_ids // b
    here = far_ids - owner * b
    devs = jnp.arange(n, dtype=jnp.int32)
    mine = owner[:, :, None] == devs
    low = jnp.min(jnp.where(mine, here[:, :, None], b - 1), axis=(0, 1))
    high = jnp.max(jnp.where(mine, here[:, :, None], 0), axis=(0, 1))
    low_of = jnp.sum(jnp.where(mine, low, 0), axis=2)
    far_rows = owner * CAP + (here > low_of).astype(jnp.int32)
    asked = lax.all_to_all(
        jnp.stack([low, high], axis=1), AXES, split_axis=0, concat_axis=0, tiled=True
    ).reshape(-1)

    vmem = pl.BlockSpec(memory_space=pltpu.VMEM)
    smem = pl.BlockSpec(memory_space=pltpu.SMEM)
    sem = pltpu.SemaphoreType.DMA((n,))
    one, two, energy = pl.pallas_call(
        functools.partial(bounce_kernel, n, lax.axis_size("gy")),
        name="bounces",
        in_specs=[smem] * 3 + [vmem] * 5,
        out_specs=[vmem] * 3,
        out_shape=[
            jax.ShapeDtypeStruct((b, ch, v), bf16),
            jax.ShapeDtypeStruct((b, ch, v), bf16),
            jax.ShapeDtypeStruct((2, 8, v), f32),
        ],
        scratch_shapes=[
            pltpu.VMEM((b, rows, v), bf16),
            pltpu.VMEM((b, GEO, v), bf16),
            pltpu.VMEM((n * CAP, GEO, v), bf16),
            pltpu.VMEM((n * CAP, GEO, v), bf16),
            pltpu.VMEM((n * CAP, rows, v), bf16),
            pltpu.VMEM((n * CAP, rows, v), bf16),
            pltpu.VMEM((n * CAP, rows, v), bf16),
            pltpu.VMEM((b, v, v), bf16),
            pltpu.VMEM((n * CAP, v, v), bf16),
            pltpu.VMEM((b, (NEAR + far) * v, v), bf16),
            pltpu.VMEM((rows, far * v), bf16),
            pltpu.VMEM((b, rows, v), f32),
            pltpu.VMEM((b, rows, v), bf16),
            pltpu.VMEM((2, 8, v), f32),
            pltpu.VMEM((2, n, 8, v), f32),
        ]
        + [sem] * 10,
        compiler_params=pltpu.CompilerParams(
            collective_id=0, has_side_effects=True, vmem_limit_bytes=VMEM_LIMIT
        ),
    )(near_rows, far_rows, asked, transfer, positions, normals, area[:, None, :], albedo)
    energies = jnp.sum(energy, axis=(1, 2)) * (1.0 / (n * b * v * ch))
    return one, two, energies


def solution(mesh):
    return jax.shard_map(
        body,
        mesh=mesh,
        in_specs=(
            P(AXES, None, None),
            P(AXES, None, None),
            P(AXES, None, None),
            P(AXES, None),
            P(AXES, None, None),
            P(AXES, None),
            P(),
        ),
        out_specs=(P(AXES, None, None), P(AXES, None, None), P()),
        check_vma=False,
    )
```

```python
import functools

import jax
import jax.numpy as jnp
from jax import lax
from jax.experimental import pallas as pl
from jax.experimental.pallas import tpu as pltpu
from jax.sharding import PartitionSpec as P

COLORS = 3
NEAR = 16
CAP = 2
AXES = ("gx", "gy")
GEO = 16
VMEM_LIMIT = 62 * 1024 * 1024
MESH = pl.DeviceIdType.MESH


def split3(f):
    hi = f.astype(jnp.bfloat16).astype(jnp.float32)
    rest = f - hi
    mid = rest.astype(jnp.bfloat16).astype(jnp.float32)
    return hi, mid, rest - mid


def source_features(pos, nrm, area):
    lanes = pos.shape[1]
    m = nrm * (area * (1.0 / jnp.pi))
    sq = jnp.sum(pos * pos, axis=0, keepdims=True)
    d = -jnp.sum(m * pos, axis=0, keepdims=True)
    feat = jnp.concatenate([pos, sq, m, d], axis=0)
    hi, mid, lo = split3(feat)
    ones = jnp.ones((8, lanes), jnp.float32)
    half = jnp.concatenate([hi, hi, hi, mid, mid, lo, ones, jnp.zeros_like(ones)], axis=0)
    return jnp.concatenate([half, half], axis=0).T


def receiver_weights(pos, nrm):
    lanes = pos.shape[1]
    zero3 = jnp.zeros((3, lanes), jnp.float32)
    zero1 = jnp.zeros((1, lanes), jnp.float32)
    one1 = jnp.ones((1, lanes), jnp.float32)
    zero5 = jnp.zeros((5, lanes), jnp.float32)
    zero8 = jnp.zeros((8, lanes), jnp.float32)

    def column(feat, const):
        hi, mid, lo = split3(feat)
        chi, cmid, clo = split3(const)
        return jnp.concatenate(
            [hi, mid, lo, hi, mid, hi, jnp.concatenate([chi, cmid, clo, zero5], axis=0), zero8],
            axis=0,
        )

    dist = column(
        jnp.concatenate([-2.0 * pos, one1, zero3, zero1], axis=0),
        jnp.sum(pos * pos, axis=0, keepdims=True) + 1.0,
    )
    along_p = column(
        jnp.concatenate([nrm, zero1, zero3, zero1], axis=0),
        -jnp.sum(nrm * pos, axis=0, keepdims=True),
    )
    along_q = column(jnp.concatenate([zero3, zero1, pos, one1], axis=0), zero1)
    return jnp.concatenate([dist, along_p, along_q], axis=1)


def block_diag(w):
    z = jnp.zeros_like(w)
    return jnp.concatenate(
        [jnp.concatenate([w, z], axis=1), jnp.concatenate([z, w], axis=1)], axis=0
    ).astype(jnp.bfloat16)


def albedo_rows(alb, rows, per_color):
    r = lax.broadcasted_iota(jnp.int32, (rows, alb.shape[1]), 0)
    out = jnp.broadcast_to(alb[COLORS - 1 : COLORS, :], (rows, alb.shape[1]))
    for c in range(COLORS - 2, -1, -1):
        out = jnp.where(r < (c + 1) * per_color, alb[c : c + 1, :], out)
    return out


def fill_table(geom, count, feats):
    def one(t, carry):
        feats[t] = source_features(*geom(t)).astype(jnp.bfloat16)
        return carry

    lax.fori_loop(0, count, one, 0)


def row_tiles(rows_ref, slot, base, weights, feats, tiles):
    v = tiles.shape[-1]
    first = lax.broadcasted_iota(jnp.int32, (v, v), 1) < v // 2
    for i in range(rows_ref.shape[1] // 4):
        t = [rows_ref[slot, i * 4 + j] for j in range(4)]
        x = jnp.concatenate(
            [
                jnp.where(first, feats[t[0]], feats[t[1]]),
                jnp.where(first, feats[t[2]], feats[t[3]]),
            ],
            axis=0,
        )
        g = jnp.dot(x, weights, preferred_element_type=jnp.float32)
        for j in range(4):
            r, c = (j // 2) * v, (j % 2) * 3 * v
            dist = g[r : r + v, c : c + v]
            ap = g[r : r + v, c + v : c + 2 * v]
            aq = g[r : r + v, c + 2 * v : c + 3 * v]
            f = jnp.maximum(ap, 0.0) * jnp.maximum(aq, 0.0) / (dist * dist)
            at = base + (i * 4 + j) * v
            tiles[slot, at : at + v, :] = f.astype(jnp.bfloat16)


def contract(rows_ref, slot, base, load, tiles):
    v = tiles.shape[-1]
    count = rows_ref.shape[1]
    picked = jnp.concatenate([load(rows_ref[slot, j]) for j in range(count)], axis=1)
    return jnp.dot(
        picked, tiles[slot, base : base + count * v, :], preferred_element_type=jnp.float32
    )


def bounce_kernel(
    n, ny,
    near_rows, far_rows, asked,
    transfer, pos, nrm, area, alb,
    one_ref, two_ref, energy_ref,
    local, geo_local, geo_out, geo_in, box_out, box_in, box_in2,
    near_feats, far_feats, tiles, acc, one, en, en_in,
    gs, gr, rs, rr, ss, sr, e1s, e1r, e2s, e2r,
):
    bf16, f32 = jnp.bfloat16, jnp.float32
    me = lax.axis_index("gx") * ny + lax.axis_index("gy")
    b, ch, v = transfer.shape
    rows = local.shape[1]
    near = near_rows.shape[1]

    def peer(d):
        t = lax.rem(me + d, n)
        return t, (t // ny, lax.rem(t, ny))

    def each_peer(fn):
        def step(d, carry):
            fn(d)
            return carry

        lax.fori_loop(1, n, step, 0)

    def copies(src, dst, send, recv):
        def make(d):
            t, dev = peer(d)
            return pltpu.make_async_remote_copy(
                src_ref=src(t), dst_ref=dst, send_sem=send.at[d], recv_sem=recv.at[d],
                device_id=dev, device_id_type=MESH,
            )

        return make

    def pair(ref, t):
        return ref.at[pl.ds(t * CAP, CAP)]

    geo_cp = copies(lambda t: pair(geo_out, t), pair(geo_in, me), gs, gr)
    rad_cp = copies(lambda t: pair(box_out, t), pair(box_in, me), rs, rr)
    sec_cp = copies(lambda t: pair(box_out, t), pair(box_in2, me), ss, sr)
    e1_cp = copies(lambda t: en.at[0], en_in.at[0, me], e1s, e1r)
    e2_cp = copies(lambda t: en.at[1], en_in.at[1, me], e2s, e2r)

    barrier = pltpu.get_barrier_semaphore()
    each_peer(lambda d: pl.semaphore_signal(barrier, inc=1, device_id=peer(d)[1], device_id_type=MESH))

    def stage(t, carry):
        local[t] = jnp.concatenate(
            [transfer[t], jnp.zeros((rows - ch, v), bf16)], axis=0
        )
        p_hi, p_mid, _ = split3(pos[t])
        n_hi, n_mid, _ = split3(nrm[t])
        geo_local[t] = jnp.concatenate(
            [p_hi, p_mid, n_hi, n_mid, area[t], jnp.zeros((GEO - 13, v), f32)], axis=0
        ).astype(bf16)
        return carry

    lax.fori_loop(0, b, stage, 0)

    def pack(source, out):
        def step(t, carry):
            for k in range(CAP):
                out[t * CAP + k] = source[asked[t * CAP + k]]
            return carry

        lax.fori_loop(0, n, step, 0)

    pack(geo_local, geo_out)
    pack(local, box_out)
    for box in (geo_in, box_in, box_in2):
        for k in range(CAP):
            box[me * CAP + k] = jnp.zeros(box.shape[1:], bf16)
    pl.semaphore_wait(barrier, n - 1)
    each_peer(lambda d: geo_cp(d).start())
    each_peer(lambda d: rad_cp(d).start())

    def weights_of(s):
        return block_diag(receiver_weights(pos[s], nrm[s]))

    fill_table(lambda t: (pos[t], nrm[t], area[t]), b, near_feats)

    def near_slot(s, carry):
        row_tiles(near_rows, s, 0, weights_of(s), near_feats, tiles)
        return carry

    def near_sum(table):
        def step(s, carry):
            acc[s] = contract(near_rows, s, 0, lambda t: table[t], tiles)
            return carry

        lax.fori_loop(0, b, step, 0, unroll=2)

    lax.fori_loop(0, b, near_slot, 0)
    near_sum(local)
    each_peer(lambda d: geo_cp(d).wait())

    def far_geom(t):
        g = geo_in[t].astype(f32)
        return g[0:3] + g[3:6], g[6:9] + g[9:12], g[12:13]

    fill_table(far_geom, n * CAP, far_feats)

    def far_slot(s, carry):
        row_tiles(far_rows, s, near * v, weights_of(s), far_feats, tiles)
        return carry

    lax.fori_loop(0, b, far_slot, 0)
    each_peer(lambda d: rad_cp(d).wait())

    def finish(s, box, e):
        total = acc[s] + contract(far_rows, s, near * v, lambda t: box[t], tiles)
        val = total * albedo_rows(alb[s], rows, ch // COLORS)
        r = lax.broadcasted_iota(jnp.int32, val.shape, 0)
        part = jnp.sum(jnp.where(r < ch, val * val * area[s], 0.0), axis=0, keepdims=True)
        return val.astype(bf16), e + part

    def first_slot(s, e):
        val, e = finish(s, box_in, e)
        one[s] = val
        one_ref[s] = val[0:ch]
        return e

    zero = jnp.zeros((1, v), f32)
    row0 = lax.broadcasted_iota(jnp.int32, (8, v), 0) == 0
    e1 = lax.fori_loop(0, b, first_slot, zero, unroll=2)
    pack(one, box_out)
    each_peer(lambda d: sec_cp(d).start())
    en[0] = jnp.where(row0, e1, 0.0)
    en_in[0, me] = en[0]

    near_sum(one)
    each_peer(lambda d: e1_cp(d).start())
    each_peer(lambda d: sec_cp(d).wait())

    def second_slot(s, e):
        val, e = finish(s, box_in2, e)
        two_ref[s] = val[0:ch]
        return e

    e2 = lax.fori_loop(0, b, second_slot, zero, unroll=2)
    en[1] = jnp.where(row0, e2, 0.0)
    en_in[1, me] = en[1]
    each_peer(lambda d: e2_cp(d).start())
    each_peer(lambda d: e1_cp(d).wait())
    each_peer(lambda d: e2_cp(d).wait())
    energy_ref[...] = jnp.sum(en_in[...], axis=1)


def body(transfer, positions, normals, area, albedo, pairs, home):
    n = lax.axis_size(AXES)
    me = lax.axis_index(AXES)
    b, ch, v = transfer.shape
    far = pairs.shape[1] - NEAR
    rows = -(-ch // 16) * 16
    bf16, f32 = jnp.bfloat16, jnp.float32

    ids = jnp.arange(home.shape[0], dtype=jnp.int32)
    slot_ids = jnp.sum(jnp.where(pairs[:, :, None] == ids, home, 0), axis=2)
    near_rows = slot_ids[:, :NEAR] - me * b
    far_ids = slot_ids[:, NEAR:]
    owner = far_ids // b
    here = far_ids - owner * b
    devs = jnp.arange(n, dtype=jnp.int32)
    mine = owner[:, :, None] == devs
    low = jnp.min(jnp.where(mine, here[:, :, None], b - 1), axis=(0, 1))
    high = jnp.max(jnp.where(mine, here[:, :, None], 0), axis=(0, 1))
    low_of = jnp.sum(jnp.where(mine, low, 0), axis=2)
    far_rows = owner * CAP + (here > low_of).astype(jnp.int32)
    asked = lax.all_to_all(
        jnp.stack([low, high], axis=1), AXES, split_axis=0, concat_axis=0, tiled=True
    ).reshape(-1)

    vmem = pl.BlockSpec(memory_space=pltpu.VMEM)
    smem = pl.BlockSpec(memory_space=pltpu.SMEM)
    sem = pltpu.SemaphoreType.DMA((n,))
    one, two, energy = pl.pallas_call(
        functools.partial(bounce_kernel, n, lax.axis_size("gy")),
        name="bounces",
        in_specs=[smem] * 3 + [vmem] * 5,
        out_specs=[vmem] * 3,
        out_shape=[
            jax.ShapeDtypeStruct((b, ch, v), bf16),
            jax.ShapeDtypeStruct((b, ch, v), bf16),
            jax.ShapeDtypeStruct((2, 8, v), f32),
        ],
        scratch_shapes=[
            pltpu.VMEM((b, rows, v), bf16),
            pltpu.VMEM((b, GEO, v), bf16),
            pltpu.VMEM((n * CAP, GEO, v), bf16),
            pltpu.VMEM((n * CAP, GEO, v), bf16),
            pltpu.VMEM((n * CAP, rows, v), bf16),
            pltpu.VMEM((n * CAP, rows, v), bf16),
            pltpu.VMEM((n * CAP, rows, v), bf16),
            pltpu.VMEM((b, v, v), bf16),
            pltpu.VMEM((n * CAP, v, v), bf16),
            pltpu.VMEM((b, (NEAR + far) * v, v), bf16),
            pltpu.VMEM((b, rows, v), f32),
            pltpu.VMEM((b, rows, v), bf16),
            pltpu.VMEM((2, 8, v), f32),
            pltpu.VMEM((2, n, 8, v), f32),
        ]
        + [sem] * 10,
        compiler_params=pltpu.CompilerParams(
            collective_id=0, has_side_effects=True, vmem_limit_bytes=VMEM_LIMIT
        ),
    )(near_rows, far_rows, asked, transfer, positions, normals, area[:, None, :], albedo)
    energies = jnp.sum(energy, axis=(1, 2)) * (1.0 / (n * b * v * ch))
    return one, two, energies


def solution(mesh):
    return jax.shard_map(
        body,
        mesh=mesh,
        in_specs=(
            P(AXES, None, None),
            P(AXES, None, None),
            P(AXES, None, None),
            P(AXES, None),
            P(AXES, None, None),
            P(AXES, None),
            P(),
        ),
        out_specs=(P(AXES, None, None), P(AXES, None, None), P()),
        check_vma=False,
    )
```
